32 devices in a mesh: outer: 8 (over z, x), inner: 4 (over y, core).
Axes of the slice: x: 2, y: 2, z: 4, core: 2. Of those that a mesh axis runs over, the one named last changes fastest.
Arguments:
- queries: bfloat16 [8192, 1024], P(('outer', 'inner')), may hold values from -10 to 10
- keys: bfloat16 [8192, 256], P(('outer', 'inner')), may hold values from -10 to 10
- values: bfloat16 [8192, 256], P(('outer', 'inner')), may hold values from -18 to 18
- pool_fine: float32 [16, 8], replicated, may hold values from -1.5 to 1.5
- pool_coarse: float32 [8, 8], replicated, may hold values from -2 to 2
- gain: float32 [1024], replicated, may hold values from 0.5 to 1.5
Outputs:
- normed: bfloat16 [8192, 1024], P(('outer', 'inner'))
The draws below stay inside these ranges and needn't reach their ends.
All inputs are finite; a program needn't handle non-finite values.
Results may differ from the reference program's by a relative error of at most 0.008.
Values may be sent and summed in bfloat16 or wider, within the bound.
A program may use at most 64 MiB of HBM per device.

```python
import jax
import jax.numpy as jnp
from jax import lax

HQ = 16
KVH = 4
HD = 64
BLOCK = 512
FINE = 16
RATIO = 8
D = 1024
COARSE = 128
GROUP = 1024
TOKENS = 8192


def joint_draw(key):
    base = jax.random.fold_in(key, 7)
    draw_q, draw_k = jax.random.split(base, 2)
    width_q = HQ * HD
    width_k = KVH * HD
    queries = jnp.clip(jax.random.normal(draw_q, (TOKENS, width_q), jnp.float32), -6.0, 6.0)
    keys = jnp.clip(jax.random.normal(draw_k, (TOKENS, width_k), jnp.float32), -6.0, 6.0)
    return (queries, keys)


def draw_queries(key, part):
    return joint_draw(key)[0].astype(jnp.bfloat16)


def draw_keys(key, part):
    return joint_draw(key)[1].astype(jnp.bfloat16)


def draw_values(key, part):
    base = jax.random.fold_in(key, 11)
    draw_v = jax.random.fold_in(base, 0)
    drawn = jnp.clip(jax.random.normal(draw_v, (TOKENS, KVH * HD), jnp.float32), -6.0, 6.0)
    return drawn.astype(jnp.bfloat16)


def noise(stream_key, extent, width, reach, held_as=jnp.bfloat16):
    entries = jax.random.normal(stream_key, extent, jnp.float32) * width
    return jnp.minimum(jnp.maximum(entries, -reach), reach).astype(held_as)


def setup_inputs(seed: int = 0) -> dict:
    key_list = jax.random.split(jax.random.key(seed), 7)
    return {
        "queries": draw_queries(jax.random.fold_in(key_list[6], 71), 0),
        "keys": draw_keys(jax.random.fold_in(key_list[6], 71), 0),
        "values": draw_values(jax.random.fold_in(key_list[6], 71), 0),
        "pool_fine": noise(key_list[3], (FINE, 2 * KVH), FINE ** -0.5, 1.5, jnp.float32),
        "pool_coarse": noise(key_list[4], (RATIO, 2 * KVH), RATIO ** -0.5, 2.0, jnp.float32),
        "gain": jnp.clip(1.0 + 0.1 * jax.random.normal(key_list[5], (D,), jnp.float32), 0.5, 1.5),
    }


EPSILON = 1e-06
MASKED_SCORE = -1e+30

def summarize(source, pooling, factor):
    amount = source.shape[0] // factor
    shaped = source.astype(jnp.float32).reshape(amount, factor, 2, KVH, HD)
    weights = pooling.astype(jnp.float32).reshape(factor, 2, KVH)
    pooled = jnp.einsum('mjskd,jsk->mskd', shaped, weights, precision=lax.Precision.HIGHEST)
    return pooled.reshape(amount, 2 * KVH * HD).astype(jnp.bfloat16)

def reference(queries, keys, values, pool_fine, pool_coarse, gain):
    paired = jnp.concatenate([keys, values], axis=1)
    fine_all = summarize(paired, pool_fine, FINE)
    coarse_all = summarize(fine_all, pool_coarse, RATIO)
    padded = jnp.pad(paired, ((BLOCK, BLOCK), (0, 0)))
    fine_group = GROUP // FINE
    coarse_pos = jnp.arange(TOKENS // COARSE, dtype=jnp.int32) * COARSE
    kv_width = KVH * HD

    def one_block(block_idx):
        first_row = (block_idx * BLOCK).astype(jnp.int32)
        query_rows = lax.dynamic_slice_in_dim(queries, first_row, BLOCK, 0)
        near = lax.dynamic_slice_in_dim(padded, first_row, 3 * BLOCK, 0)
        near_pos = first_row - BLOCK + jnp.arange(3 * BLOCK, dtype=jnp.int32)
        near_ok = (near_pos >= 0) & (near_pos < TOKENS)
        group_idx = (first_row // GROUP).astype(jnp.int32)
        fine_rows = lax.dynamic_slice_in_dim(fine_all, (group_idx * fine_group).astype(jnp.int32), fine_group, 0)
        fine_pos = group_idx * GROUP + jnp.arange(fine_group, dtype=jnp.int32) * FINE
        fine_ok = jnp.abs(fine_pos // BLOCK - block_idx) > 1
        coarse_ok = (coarse_pos // GROUP != group_idx) & (jnp.abs(coarse_pos // BLOCK - block_idx) > 1)
        keyset = jnp.concatenate([near, fine_rows, coarse_all], axis=0)
        allowed = jnp.concatenate([near_ok, fine_ok, coarse_ok])
        amount = keyset.shape[0]
        key_heads = keyset[:, :kv_width].astype(jnp.float32).reshape(amount, KVH, HD)
        value_heads = keyset[:, kv_width:].astype(jnp.float32).reshape(amount, KVH, HD)
        query_heads = query_rows.astype(jnp.float32).reshape(BLOCK, KVH, HQ // KVH, HD)
        scores = jnp.einsum('qgrd,kgd->grqk', query_heads, key_heads, precision=lax.Precision.HIGHEST) * HD ** (-0.5)
        scores = jnp.where(allowed, scores, MASKED_SCORE)
        peak = lax.optimization_barrier(jnp.max(scores, axis=3, keepdims=True))
        expon = jnp.where(allowed, jnp.exp(scores - peak), 0.0)
        totals = lax.optimization_barrier(jnp.sum(expon, axis=3))
        rounded = lax.optimization_barrier(expon.astype(jnp.bfloat16)).astype(jnp.float32)
        blended = jnp.einsum('grqk,kgd->qgrd', rounded, value_heads, precision=lax.Precision.HIGHEST)
        attended = blended / jnp.transpose(totals, (2, 0, 1))[..., None]
        return attended.reshape(BLOCK, HQ * HD)
    attended = lax.map(one_block, jnp.arange(TOKENS // BLOCK, dtype=jnp.int32)).reshape(TOKENS, HQ * HD)
    rescale = lax.rsqrt(lax.optimization_barrier(jnp.mean(attended * attended, axis=1, keepdims=True)) + EPSILON)
    return (attended * rescale * gain).astype(jnp.bfloat16)
```

```python
import functools
import math

import jax
import jax.numpy as jnp
from jax import lax
from jax.experimental import pallas as pl
from jax.experimental.pallas import tpu as pltpu
from jax.sharding import PartitionSpec as P

HQ = 16
KVH = 4
HD = 64
BLOCK = 512
FINE = 16
RATIO = 8
COARSE = 128

EPSILON = 1e-06
MASKED_SCORE = -1e30
LANES = 128
MESH = pl.DeviceIdType.MESH
BF16 = jnp.bfloat16
F32 = jnp.float32


def kernel(
    outer_count, inner_count,
    q_ref, k_ref, v_ref, pf_ref, pc_ref, gain_ref, out_ref,
    q_all, own_k, own_v, mate_k, mate_v, other_k, other_v,
    ka, va, kb, vb, kc, vc, bias_ref,
    fine_send, fine_all, coarse_send, coarse_pad, coarse_group, coarse_all,
    peaks, sums, att_own, att_send, att_recv,
    q_ss, q_rs, own_ss, own_rs, mate_ss, mate_rs, other_ss, other_rs,
    fine_ss, fine_rs, cg_ss, cg_rs, co_ss, co_rs, att_ss, att_rs,
):
    tok = q_ref.shape[0]
    ranks = BLOCK // tok
    kv_width = KVH * HD
    share = kv_width // ranks
    q_share = HQ * HD // ranks
    tiles = q_share // LANES
    kv_local = share // HD
    tiles_per_kv = tiles // kv_local
    fine_dev = tok // FINE
    coarse_dev = tok // COARSE
    group_tok = tok * inner_count
    fine_amount = group_tok // FINE
    coarse_amount = outer_count * group_tok // COARSE
    blocks = outer_count * inner_count // ranks
    factor = HD ** (-0.5) * math.log2(math.e)

    o_me = lax.axis_index("outer")
    i_me = lax.axis_index("inner")
    linear = o_me * inner_count + i_me
    block = linear // ranks
    rank = lax.rem(linear, ranks)
    odd = lax.rem(block, 2)
    mate = block + 1 - 2 * odd
    other = block - 1 + 2 * odd
    has_other = (other >= 0) & (other < blocks)

    def at_rank(which_block, rel):
        target_rank = lax.rem(rank + rel, ranks)
        spot = which_block * ranks + target_rank
        return (spot // inner_count, lax.rem(spot, inner_count)), target_rank

    inner_peers = [lax.rem(i_me + rel, inner_count) for rel in range(1, inner_count)]
    outer_peers = [lax.rem(o_me + rel, outer_count) for rel in range(1, outer_count)]

    barrier = pltpu.get_barrier_semaphore()

    def greet(device):
        pl.semaphore_signal(barrier, inc=1, device_id=device, device_id_type=MESH)

    for peer in inner_peers:
        greet((o_me, peer))
    for peer in outer_peers:
        greet((peer, i_me))
    for rel in range(ranks):
        greet(at_rank(mate, rel)[0])

    for rel in range(ranks):
        greet(at_rank(lax.rem(other + blocks, blocks), rel)[0])
    pl.semaphore_wait(barrier, inner_count - 1 + outer_count - 1 + 2 * ranks)

    def remote(src, dst, send_sem, recv_sem, device):
        return pltpu.make_async_remote_copy(
            src_ref=src, dst_ref=dst, send_sem=send_sem, recv_sem=recv_sem,
            device_id=device, device_id_type=MESH,
        )

    def cols(index, width):
        return pl.ds(pl.multiple_of(index * width, LANES), width)

    own_copies = []
    for rel in range(1, ranks):
        device, target = at_rank(block, rel)
        slot = ranks - rel
        own_copies.append(remote(
            k_ref.at[:, cols(target, share)], own_k.at[slot],
            own_ss.at[0, slot], own_rs.at[0, slot], device))
        own_copies.append(remote(
            q_ref.at[:, cols(target, q_share)], q_all.at[slot],
            q_ss.at[slot], q_rs.at[slot], device))
        own_copies.append(remote(
            v_ref.at[:, cols(target, share)], own_v.at[slot],
            own_ss.at[1, slot], own_rs.at[1, slot], device))
    for copy in own_copies:
        copy.start()

    def block_copies(which, k_dst, v_dst, ss, rs):
        made = []
        for part, (src, dst) in enumerate(((k_ref, k_dst), (v_ref, v_dst))):
            for rel in range(ranks):
                device, target = at_rank(which, rel)
                slot = (ranks - rel) % ranks
                made.append(remote(
                    src.at[:, cols(target, share)], dst.at[slot],
                    ss.at[part, slot], rs.at[part, slot], device))
        return made

    mate_copies = block_copies(mate, mate_k, mate_v, mate_ss, mate_rs)
    for copy in mate_copies:
        copy.start()

    @pl.when(has_other)
    def _():
        for copy in block_copies(other, other_k, other_v, other_ss, other_rs):
            copy.start()

    def spread(pool_ref):
        rows = pool_ref.shape[0]
        pool = pool_ref[...]
        return jnp.concatenate(
            [jnp.broadcast_to(pool[:, n:n + 1], (rows, HD)) for n in range(2 * KVH)], axis=1)

    pf = spread(pf_ref)
    pc = spread(pc_ref)
    paired = jnp.concatenate([k_ref[...], v_ref[...]], axis=1).astype(F32)
    fine = jnp.sum(paired.reshape(fine_dev, FINE, 2 * kv_width) * pf[None], axis=1).astype(BF16)
    fine_wide = fine.astype(F32)
    coarse = jnp.sum(
        fine_wide.reshape(coarse_dev, RATIO, 2 * kv_width) * pc[None], axis=1).astype(BF16)
    padded = -(-coarse_dev // 8) * 8
    coarse_wide = coarse.astype(F32)
    if padded > coarse_dev:
        coarse_wide = jnp.concatenate(
            [coarse_wide, jnp.zeros((padded - coarse_dev, 2 * kv_width), F32)], axis=0)
    for n in range(ranks):
        k_cols = slice(n * share, (n + 1) * share)
        v_cols = slice(kv_width + n * share, kv_width + (n + 1) * share)
        fine_send[n] = jnp.concatenate([fine[:, k_cols], fine[:, v_cols]], axis=1)
        coarse_send[n] = jnp.concatenate([coarse_wide[:, k_cols], coarse_wide[:, v_cols]], axis=1)
    fine_all[i_me] = fine_send[rank]
    coarse_pad[i_me] = coarse_send[rank]

    group_copies = []
    for n, peer in enumerate(inner_peers):
        peer_rank = lax.rem(peer, ranks)
        group_copies.append(remote(
            coarse_send.at[peer_rank], coarse_pad.at[i_me],
            cg_ss.at[n], cg_rs.at[n], (o_me, peer)))
        group_copies.append(remote(
            fine_send.at[peer_rank], fine_all.at[i_me],
            fine_ss.at[n], fine_rs.at[n], (o_me, peer)))
    for copy in group_copies:
        copy.start()

    low = (lax.broadcasted_iota(jnp.int32, (1, LANES), 1) < HD).astype(F32).astype(BF16)
    high = (lax.broadcasted_iota(jnp.int32, (1, LANES), 1) >= HD).astype(F32).astype(BF16)

    def variants(k_raw, v_raw, k_out, v_out, rows):
        k_swap = pltpu.roll(k_raw.astype(F32), HD, 1).astype(BF16)
        v_swap = pltpu.roll(v_raw.astype(F32), HD, 1).astype(BF16)
        for n in range(kv_local):
            at_low = (k_raw, v_raw) if n == 0 else (k_swap, v_swap)
            at_high = (k_swap, v_swap) if n == 0 else (k_raw, v_raw)
            k_out[n, 0, rows, :] = at_low[0] * low
            k_out[n, 1, rows, :] = at_high[0] * high
            v_out[n, 0, rows, :] = at_low[1] * low + high
            v_out[n, 1, rows, :] = at_high[1] * high + low

    q_all[0] = q_ref[:, cols(rank, q_share)]
    variants(k_ref[:, cols(rank, share)], v_ref[:, cols(rank, share)], ka, va, slice(0, tok))
    for copy in own_copies:
        copy.wait_recv()
    for slot in range(1, ranks):
        variants(own_k[slot], own_v[slot], ka, va, slice(slot * tok, (slot + 1) * tok))

    def unit(part, tile, half, k_set, v_set, bias, first):
        n = tile // tiles_per_kv
        query = q_all[part, :, cols(tile, LANES)]
        scores = lax.dot_general(
            query, k_set[n, half], (((1,), (1,)), ((), ())), preferred_element_type=F32)
        if bias is not None:
            scores = scores + bias
        peak = jnp.max(scores, axis=1, keepdims=True)
        at = (part * tiles + tile) * 2 + half
        if not first:
            before = peaks[at][:, :1]
            peak = jnp.maximum(peak, before)
        weights = jnp.exp2((scores - peak) * factor).astype(BF16)
        blended = jnp.dot(weights, v_set[n, half], preferred_element_type=F32)
        if not first:
            blended = blended + sums[at] * jnp.exp2((before - peak) * factor)
        return at, peak, blended

    def stage(parts, k_set, v_set, first):
        def body(step, carry):
            part = step // tiles
            tile = lax.rem(step, tiles)
            done = [unit(part, tile, half, k_set, v_set, None, first) for half in range(2)]
            for at, peak, blended in done:
                peaks[at] = jnp.broadcast_to(peak, (tok, LANES))
                sums[at] = blended
            return carry
        lax.fori_loop(0, parts * tiles, body, 0)

    stage(ranks, ka, va, True)

    for copy in group_copies:
        copy.wait_recv()
    for n in range(inner_count):
        coarse_group[n * coarse_dev:(n + 1) * coarse_dev, :] = coarse_pad[n, 0:coarse_dev, :]
    coarse_all[o_me] = coarse_group[...]
    outer_copies = []
    for n, peer in enumerate(outer_peers):
        outer_copies.append(remote(
            coarse_group, coarse_all.at[o_me], co_ss.at[n], co_rs.at[n], (peer, i_me)))
    for copy in outer_copies:
        copy.start()

    for copy in mate_copies:
        copy.wait_recv()
    for slot in range(ranks):
        variants(mate_k[slot], mate_v[slot], kb, vb, slice(slot * tok, (slot + 1) * tok))
    stage(ranks, kb, vb, False)

    for copy in outer_copies:
        copy.wait_recv()
    fine_rows = fine_all[...].reshape(fine_amount, 2 * share)
    variants(fine_rows[:, :share], fine_rows[:, share:], kc, vc, slice(BLOCK, BLOCK + fine_amount))
    coarse_rows = coarse_all[...].reshape(coarse_amount, 2 * share).astype(BF16)
    variants(coarse_rows[:, :share], coarse_rows[:, share:], kc, vc,
             slice(BLOCK + fine_amount, BLOCK + fine_amount + coarse_amount))
    far = fine_amount + coarse_amount
    spot = lax.broadcasted_iota(jnp.int32, (1, far), 1)
    fine_pos = o_me * group_tok + spot * FINE
    coarse_pos = (spot - fine_amount) * COARSE
    position = jnp.where(spot < fine_amount, fine_pos, coarse_pos)
    distance = jnp.abs(lax.div(position, BLOCK) - block)
    outside = (spot < fine_amount) | (lax.div(position, group_tok) != o_me)
    bias_ref[:, BLOCK:] = jnp.where((distance > 1) & outside, 0.0, MASKED_SCORE)

    @pl.when(has_other)
    def _():
        for copy in block_copies(other, other_k, other_v, other_ss, other_rs):
            copy.wait_recv()
        for slot in range(ranks):
            variants(other_k[slot], other_v[slot], kc, vc, slice(slot * tok, (slot + 1) * tok))
        bias_ref[:, :BLOCK] = jnp.zeros((1, BLOCK), F32)

    @pl.when(jnp.logical_not(has_other))
    def _():
        zero = jnp.zeros((BLOCK, LANES), BF16)
        for n in range(kv_local):
            for half in range(2):
                kc[n, half, 0:BLOCK, :] = zero
                vc[n, half, 0:BLOCK, :] = zero
        bias_ref[:, :BLOCK] = jnp.full((1, BLOCK), MASKED_SCORE, F32)

    is_low = lax.broadcasted_iota(jnp.int32, (1, LANES), 1) < HD

    def finish(part, tile):
        bias = bias_ref[...]
        lower, upper = [unit(part, tile, half, kc, vc, bias, False)[2] for half in range(2)]
        totals = pltpu.roll(jnp.where(is_low, upper, lower), HD, 1)
        return jnp.where(is_low, lower, upper) / totals

    def att_copy(part, tile):
        device, _ = at_rank(block, part)
        slot = ranks - part - 1
        return remote(att_send.at[part - 1, tile], att_recv.at[slot, tile],
                      att_ss.at[slot, tile], att_rs.at[slot, tile], device)

    for part in range(1, ranks):
        def give(tile, carry):
            att_send[part - 1, tile] = finish(part, tile)
            att_copy(part, tile).start()
            return carry
        lax.fori_loop(0, tiles, give, 0)

    def keep(tile, square):
        attended = finish(0, tile)
        att_own[tile] = attended
        return square + attended * attended

    square = lax.fori_loop(0, tiles, keep, jnp.zeros((tok, LANES), F32))
    for part in range(1, ranks):
        for tile in range(tiles):
            att_copy(part, tile).wait_recv()
            attended = att_recv[ranks - part - 1, tile]
            square = square + attended * attended
    rescale = lax.rsqrt(jnp.sum(square, axis=1, keepdims=True) / (HQ * HD) + EPSILON)
    for slot in range(ranks):
        column = lax.rem(rank + slot, ranks) * tiles
        for tile in range(tiles):
            attended = att_own[tile] if slot == 0 else att_recv[slot - 1, tile]
            where = cols(column + tile, LANES)
            out_ref[:, where] = (attended * rescale * gain_ref[:, where]).astype(BF16)

    for copy in own_copies + mate_copies + group_copies + outer_copies:
        copy.wait_send()

    @pl.when(has_other)
    def _():
        for copy in block_copies(other, other_k, other_v, other_ss, other_rs):
            copy.wait_send()

    for part in range(1, ranks):
        for tile in range(tiles):
            att_copy(part, tile).wait_send()


def local(outer_count, inner_count, queries, keys, values, pool_fine, pool_coarse, gain):
    tok = queries.shape[0]
    ranks = BLOCK // tok
    share = KVH * HD // ranks
    kv_local = share // HD
    q_share = HQ * HD // ranks
    tiles = q_share // LANES
    group_tok = tok * inner_count
    far = group_tok // FINE + outer_count * group_tok // COARSE
    coarse_dev = tok // COARSE
    padded = -(-coarse_dev // 8) * 8
    assert ranks >= 2 and BLOCK % tok == 0 and kv_local == 2 and share == LANES
    assert inner_count % ranks == 0 and (outer_count * inner_count // ranks) % 2 == 0
    dma = pltpu.SemaphoreType.DMA
    vmem = pltpu.VMEM
    near = lambda: vmem((ranks, tok, share), BF16)
    sets = lambda amount: vmem((kv_local, 2, amount, LANES), BF16)
    units = ranks * tiles * 2
    pair = lambda: dma((2, ranks))
    return pl.pallas_call(
        functools.partial(kernel, outer_count, inner_count),
        out_shape=jax.ShapeDtypeStruct((tok, HQ * HD), BF16),
        in_specs=[pl.BlockSpec(memory_space=pltpu.VMEM)] * 6,
        out_specs=pl.BlockSpec(memory_space=pltpu.VMEM),
        scratch_shapes=[
            vmem((ranks, tok, q_share), BF16),
            near(), near(), near(), near(), near(), near(),
            sets(BLOCK), sets(BLOCK), sets(BLOCK), sets(BLOCK),
            sets(BLOCK + far), sets(BLOCK + far), vmem((1, BLOCK + far), F32),
            vmem((ranks, tok // FINE, 2 * share), BF16),
            vmem((inner_count, tok // FINE, 2 * share), BF16),
            vmem((ranks, padded, 2 * share), F32),
            vmem((inner_count, padded, 2 * share), F32),
            vmem((inner_count * coarse_dev, 2 * share), F32),
            vmem((outer_count, inner_count * coarse_dev, 2 * share), F32),
            vmem((units, tok, LANES), F32),
            vmem((units, tok, LANES), F32),
            vmem((tiles, tok, LANES), F32),
            vmem((ranks - 1, tiles, tok, LANES), F32),
            vmem((ranks - 1, tiles, tok, LANES), F32),
            dma((ranks,)), dma((ranks,)),
            pair(), pair(), pair(), pair(), pair(), pair(),
            dma((inner_count - 1,)), dma((inner_count - 1,)),
            dma((inner_count - 1,)), dma((inner_count - 1,)),
            dma((outer_count - 1,)), dma((outer_count - 1,)),
            dma((ranks - 1, tiles)), dma((ranks - 1, tiles)),
        ],
        compiler_params=pltpu.CompilerParams(
            collective_id=0, has_side_effects=True, vmem_limit_bytes=56 * 1024 * 1024),
    )(queries, keys, values, pool_fine, pool_coarse, gain.reshape(1, -1))


def solution(mesh):
    rows = P(("outer", "inner"), None)
    return jax.shard_map(
        functools.partial(local, mesh.shape["outer"], mesh.shape["inner"]),
        mesh=mesh, in_specs=(rows, rows, rows, P(), P(), P()),
        out_specs=rows, check_vma=False,
    )
```

```python
import functools
import math

import jax
import jax.numpy as jnp
from jax import lax
from jax.experimental import pallas as pl
from jax.experimental.pallas import tpu as pltpu
from jax.sharding import PartitionSpec as P

HQ = 16
KVH = 4
HD = 64
BLOCK = 512
FINE = 16
RATIO = 8
COARSE = 128

EPSILON = 1e-06
MASKED_SCORE = -1e30
LANES = 128
MESH = pl.DeviceIdType.MESH
BF16 = jnp.bfloat16
F32 = jnp.float32


def kernel(
    outer_count, inner_count,
    q_hbm, k_hbm, v_hbm, pf_hbm, pc_hbm, out_ref,
    q_ref, k_ref, v_ref, pf_ref, pc_ref, in_sems,
    q_all, own_k, own_v, mate_k, mate_v, other_k, other_v,
    ka, va, kb, vb, kc, vc, bias_ref,
    fine_send, fine_all, coarse_send, coarse_pad, coarse_group, coarse_all,
    peaks, sums, att_send, att_recv,
    q_ss, q_rs, own_ss, own_rs, mate_ss, mate_rs, other_ss, other_rs,
    fine_ss, fine_rs, cg_ss, cg_rs, co_ss, co_rs, att_ss, att_rs,
):
    tok = q_ref.shape[0]
    ranks = BLOCK // tok
    kv_width = KVH * HD
    share = kv_width // ranks
    q_share = HQ * HD // ranks
    tiles = q_share // LANES
    kv_local = share // HD
    tiles_per_kv = tiles // kv_local
    fine_dev = tok // FINE
    coarse_dev = tok // COARSE
    group_tok = tok * inner_count
    fine_amount = group_tok // FINE
    coarse_amount = outer_count * group_tok // COARSE
    blocks = outer_count * inner_count // ranks
    factor = HD ** (-0.5) * math.log2(math.e)

    o_me = lax.axis_index("outer")
    i_me = lax.axis_index("inner")
    linear = o_me * inner_count + i_me
    block = linear // ranks
    rank = lax.rem(linear, ranks)
    odd = lax.rem(block, 2)
    mate = block + 1 - 2 * odd
    relay_from = block - 2 + 4 * odd
    relay_to = block + 2 - 4 * odd
    has_other = (relay_from >= 0) & (relay_from < blocks)
    has_next = (relay_to >= 0) & (relay_to < blocks)

    def at_rank(which_block, rel):
        target_rank = lax.rem(rank + rel, ranks)
        spot = which_block * ranks + target_rank
        return (spot // inner_count, lax.rem(spot, inner_count)), target_rank

    inner_peers = [lax.rem(i_me + rel, inner_count) for rel in range(1, inner_count)]
    outer_peers = [lax.rem(o_me + rel, outer_count) for rel in range(1, outer_count)]

    loads = [
        pltpu.make_async_copy(src, dst, in_sems.at[n])
        for n, (src, dst) in enumerate((
            (k_hbm, k_ref), (q_hbm, q_ref), (v_hbm, v_ref), (pf_hbm, pf_ref), (pc_hbm, pc_ref)))
    ]
    for load in loads:
        load.start()

    barrier = pltpu.get_barrier_semaphore()

    def greet(device):
        pl.semaphore_signal(barrier, inc=1, device_id=device, device_id_type=MESH)

    for peer in inner_peers:
        greet((o_me, peer))
    for peer in outer_peers:
        greet((peer, i_me))
    for rel in range(ranks):
        greet(at_rank(mate, rel)[0])

    for which in (relay_from, relay_to):
        greet(at_rank(lax.rem(which + blocks, blocks), 0)[0])
    pl.semaphore_wait(barrier, inner_count - 1 + outer_count - 1 + ranks + 2)

    for load in loads:
        load.wait()

    def remote(src, dst, send_sem, recv_sem, device):
        return pltpu.make_async_remote_copy(
            src_ref=src, dst_ref=dst, send_sem=send_sem, recv_sem=recv_sem,
            device_id=device, device_id_type=MESH,
        )

    def cols(index, width):
        return pl.ds(pl.multiple_of(index * width, LANES), width)

    own_copies = []
    for rel in range(1, ranks):
        device, target = at_rank(block, rel)
        slot = ranks - rel
        own_copies.append(remote(
            k_ref.at[:, cols(target, share)], own_k.at[slot],
            own_ss.at[0, slot], own_rs.at[0, slot], device))
        own_copies.append(remote(
            q_ref.at[:, cols(target, q_share)], q_all.at[slot],
            q_ss.at[slot], q_rs.at[slot], device))
        own_copies.append(remote(
            v_ref.at[:, cols(target, share)], own_v.at[slot],
            own_ss.at[1, slot], own_rs.at[1, slot], device))
    for copy in own_copies:
        copy.start()

    def mate_copies_of(part, src, dst):
        made = []
        for rel in range(ranks):
            device, target = at_rank(mate, rel)
            slot = (ranks - rel) % ranks
            made.append(remote(
                src.at[:, cols(target, share)], dst.at[slot],
                mate_ss.at[part, slot], mate_rs.at[part, slot], device))
        return made

    def relay_copies(part):
        device = at_rank(relay_to, 0)[0]
        src, dst = ((mate_k, other_k), (mate_v, other_v))[part]
        return [remote(src.at[slot], dst.at[slot], other_ss.at[part, slot],
                       other_rs.at[part, slot], device) for slot in range(ranks)]

    mate_k_copies = mate_copies_of(0, k_ref, mate_k)
    mate_v_copies = mate_copies_of(1, v_ref, mate_v)
    for copy in mate_k_copies:
        copy.start()

    def spread(pool):
        rows = pool.shape[0]
        return jnp.concatenate(
            [jnp.broadcast_to(pool[:, n:n + 1], (rows, HD)) for n in range(2 * KVH)], axis=1)

    pf = spread(pf_ref[...].T)
    pc = spread(pc_ref[...])
    paired = jnp.concatenate([k_ref[...], v_ref[...]], axis=1).astype(F32)
    fine = jnp.sum(paired.reshape(fine_dev, FINE, 2 * kv_width) * pf[None], axis=1).astype(BF16)
    fine_wide = fine.astype(F32)
    coarse = jnp.sum(
        fine_wide.reshape(coarse_dev, RATIO, 2 * kv_width) * pc[None], axis=1).astype(BF16)
    padded = -(-coarse_dev // 8) * 8
    coarse_wide = coarse.astype(F32)
    if padded > coarse_dev:
        coarse_wide = jnp.concatenate(
            [coarse_wide, jnp.zeros((padded - coarse_dev, 2 * kv_width), F32)], axis=0)
    for n in range(ranks):
        k_cols = slice(n * share, (n + 1) * share)
        v_cols = slice(kv_width + n * share, kv_width + (n + 1) * share)
        fine_send[n] = jnp.concatenate([fine[:, k_cols], fine[:, v_cols]], axis=1)
        coarse_send[n] = jnp.concatenate([coarse_wide[:, k_cols], coarse_wide[:, v_cols]], axis=1)
    fine_all[i_me] = fine_send[rank]
    coarse_pad[i_me] = coarse_send[rank]

    group_copies = []
    for n, peer in enumerate(inner_peers):
        peer_rank = lax.rem(peer, ranks)
        group_copies.append(remote(
            coarse_send.at[peer_rank], coarse_pad.at[i_me],
            cg_ss.at[n], cg_rs.at[n], (o_me, peer)))
        group_copies.append(remote(
            fine_send.at[peer_rank], fine_all.at[i_me],
            fine_ss.at[n], fine_rs.at[n], (o_me, peer)))
    for copy in group_copies + mate_v_copies:
        copy.start()

    low = (lax.broadcasted_iota(jnp.int32, (1, LANES), 1) < HD).astype(F32).astype(BF16)
    high = (lax.broadcasted_iota(jnp.int32, (1, LANES), 1) >= HD).astype(F32).astype(BF16)

    def variants(k_raw, v_raw, k_out, v_out, rows):
        k_swap = pltpu.roll(k_raw.astype(F32), HD, 1).astype(BF16)
        v_swap = pltpu.roll(v_raw.astype(F32), HD, 1).astype(BF16)
        for n in range(kv_local):
            at_low = (k_raw, v_raw) if n == 0 else (k_swap, v_swap)
            at_high = (k_swap, v_swap) if n == 0 else (k_raw, v_raw)
            k_out[n, 0, rows, :] = at_low[0] * low
            k_out[n, 1, rows, :] = at_high[0] * high
            v_out[n, 0, rows, :] = at_low[1] * low + high
            v_out[n, 1, rows, :] = at_high[1] * high + low

    q_all[0] = q_ref[:, cols(rank, q_share)]
    variants(k_ref[:, cols(rank, share)], v_ref[:, cols(rank, share)], ka, va, slice(0, tok))
    for copy in own_copies:
        copy.wait_recv()
    for slot in range(1, ranks):
        variants(own_k[slot], own_v[slot], ka, va, slice(slot * tok, (slot + 1) * tok))

    def unit(part, tile, half, k_set, v_set, bias, first):
        n = tile // tiles_per_kv
        query = q_all[part, :, cols(tile, LANES)]
        scores = lax.dot_general(
            query, k_set[n, half], (((1,), (1,)), ((), ())), preferred_element_type=F32)
        if bias is not None:
            scores = scores + bias
        peak = jnp.max(scores, axis=1, keepdims=True)
        at = (part * tiles + tile) * 2 + half
        peak = jnp.broadcast_to(peak, (tok, LANES))
        if not first:
            before = peaks[at]
            peak = jnp.maximum(peak, before)
        wide = jnp.concatenate([peak] * (scores.shape[1] // LANES), axis=1)
        weights = jnp.exp2((scores - wide) * factor).astype(BF16)
        blended = jnp.dot(weights, v_set[n, half], preferred_element_type=F32)
        if not first:
            blended = blended + sums[at] * jnp.exp2((before - peak) * factor)
        return at, peak, blended

    def stage(parts, k_set, v_set, first):
        def body(step, carry):
            part = step // tiles
            tile = lax.rem(step, tiles)
            done = [unit(part, tile, half, k_set, v_set, None, first) for half in range(2)]
            for at, peak, blended in done:
                peaks[at] = peak
                sums[at] = blended
            return carry
        lax.fori_loop(0, parts * tiles, body, 0)

    stage(ranks, ka, va, True)

    for copy in group_copies:
        copy.wait_recv()
    for n in range(inner_count):
        coarse_group[n * coarse_dev:(n + 1) * coarse_dev, :] = coarse_pad[n, 0:coarse_dev, :]
    coarse_all[o_me] = coarse_group[...]
    outer_copies = []
    for n, peer in enumerate(outer_peers):
        outer_copies.append(remote(
            coarse_group, coarse_all.at[o_me], co_ss.at[n], co_rs.at[n], (peer, i_me)))
    for copy in outer_copies:
        copy.start()

    for part, copies in enumerate((mate_k_copies, mate_v_copies)):
        for copy in copies:
            copy.wait_recv()

        @pl.when(has_next)
        def _():
            for copy in relay_copies(part):
                copy.start()
    for slot in range(ranks):
        variants(mate_k[slot], mate_v[slot], kb, vb, slice(slot * tok, (slot + 1) * tok))
    stage(ranks, kb, vb, False)

    for copy in outer_copies:
        copy.wait_recv()
    fine_rows = fine_all[...].reshape(fine_amount, 2 * share)
    variants(fine_rows[:, :share], fine_rows[:, share:], kc, vc, slice(BLOCK, BLOCK + fine_amount))
    coarse_rows = coarse_all[...].reshape(coarse_amount, 2 * share).astype(BF16)
    variants(coarse_rows[:, :share], coarse_rows[:, share:], kc, vc,
             slice(BLOCK + fine_amount, BLOCK + fine_amount + coarse_amount))
    far = fine_amount + coarse_amount
    spot = lax.broadcasted_iota(jnp.int32, (1, far), 1)
    fine_pos = o_me * group_tok + spot * FINE
    coarse_pos = (spot - fine_amount) * COARSE
    position = jnp.where(spot < fine_amount, fine_pos, coarse_pos)
    distance = jnp.abs(lax.div(position, BLOCK) - block)
    outside = (spot < fine_amount) | (lax.div(position, group_tok) != o_me)
    bias_ref[:, BLOCK:] = jnp.where((distance > 1) & outside, 0.0, MASKED_SCORE)

    @pl.when(has_other)
    def _():
        for copy in relay_copies(0) + relay_copies(1):
            copy.wait_recv()
        for slot in range(ranks):
            variants(other_k[slot], other_v[slot], kc, vc, slice(slot * tok, (slot + 1) * tok))
        bias_ref[:, :BLOCK] = jnp.zeros((1, BLOCK), F32)

    @pl.when(jnp.logical_not(has_other))
    def _():
        zero = jnp.zeros((BLOCK, LANES), BF16)
        for n in range(kv_local):
            for half in range(2):
                kc[n, half, 0:BLOCK, :] = zero
                vc[n, half, 0:BLOCK, :] = zero
        bias_ref[:, :BLOCK] = jnp.full((1, BLOCK), MASKED_SCORE, F32)

    is_low = lax.broadcasted_iota(jnp.int32, (1, LANES), 1) < HD

    def finish(part, tile):
        bias = bias_ref[...]
        lower, upper = [unit(part, tile, half, kc, vc, bias, False)[2] for half in range(2)]
        totals = pltpu.roll(jnp.where(is_low, upper, lower), HD, 1)
        return jnp.where(is_low, lower, upper) / totals

    def att_copy(part, tile):
        device, _ = at_rank(block, part)
        slot = ranks - part - 1
        return remote(att_send.at[part - 1, tile], att_recv.at[slot, tile],
                      att_ss.at[slot, tile], att_rs.at[slot, tile], device)

    for part in range(1, ranks):
        def give(tile, carry):
            att_send[part - 1, tile] = finish(part, tile)
            att_copy(part, tile).start()
            return carry
        lax.fori_loop(0, tiles, give, 0)

    def keep(tile, carry):
        out_ref[:, cols(rank * tiles + tile, LANES)] = finish(0, tile)
        return carry

    lax.fori_loop(0, tiles, keep, 0)
    for part in range(1, ranks):
        slot = ranks - part
        column = lax.rem(rank + slot, ranks) * tiles
        for tile in range(tiles):
            att_copy(part, tile).wait_recv()
            out_ref[:, cols(column + tile, LANES)] = att_recv[slot - 1, tile]

    for copy in own_copies + mate_k_copies + mate_v_copies + group_copies + outer_copies:
        copy.wait_send()

    @pl.when(has_next)
    def _():
        for copy in relay_copies(0) + relay_copies(1):
            copy.wait_send()

    for part in range(1, ranks):
        for tile in range(tiles):
            att_copy(part, tile).wait_send()


def norm_kernel(attended_ref, gain_ref, out_ref):
    attended = attended_ref[...]
    rescale = lax.rsqrt(jnp.mean(attended * attended, axis=1, keepdims=True) + EPSILON)
    out_ref[...] = (attended * rescale * gain_ref[...]).astype(BF16)


def local(outer_count, inner_count, queries, keys, values, pool_fine, pool_coarse, gain):
    tok = queries.shape[0]
    ranks = BLOCK // tok
    share = KVH * HD // ranks
    kv_local = share // HD
    q_share = HQ * HD // ranks
    tiles = q_share // LANES
    group_tok = tok * inner_count
    far = group_tok // FINE + outer_count * group_tok // COARSE
    coarse_dev = tok // COARSE
    padded = -(-coarse_dev // 8) * 8
    assert ranks >= 2 and BLOCK % tok == 0 and kv_local == 2 and share == LANES
    assert inner_count % ranks == 0 and (outer_count * inner_count // ranks) % 2 == 0
    dma = pltpu.SemaphoreType.DMA
    vmem = pltpu.VMEM
    near = lambda: vmem((ranks, tok, share), BF16)
    sets = lambda amount: vmem((kv_local, 2, amount, LANES), BF16)
    units = ranks * tiles * 2
    pair = lambda: dma((2, ranks))
    attended = pl.pallas_call(
        functools.partial(kernel, outer_count, inner_count),
        out_shape=jax.ShapeDtypeStruct((tok, HQ * HD), F32),
        in_specs=[pl.BlockSpec(memory_space=pltpu.HBM)] * 5,
        out_specs=pl.BlockSpec(memory_space=pltpu.VMEM),
        scratch_shapes=[
            vmem(queries.shape, BF16), vmem(keys.shape, BF16), vmem(values.shape, BF16),
            vmem(pool_fine.shape[::-1], F32), vmem(pool_coarse.shape, F32), dma((5,)),
            vmem((ranks, tok, q_share), BF16),
            near(), near(), near(), near(), near(), near(),
            sets(BLOCK), sets(BLOCK), sets(BLOCK), sets(BLOCK),
            sets(BLOCK + far), sets(BLOCK + far), vmem((1, BLOCK + far), F32),
            vmem((ranks, tok // FINE, 2 * share), BF16),
            vmem((inner_count, tok // FINE, 2 * share), BF16),
            vmem((ranks, padded, 2 * share), F32),
            vmem((inner_count, padded, 2 * share), F32),
            vmem((inner_count * coarse_dev, 2 * share), F32),
            vmem((outer_count, inner_count * coarse_dev, 2 * share), F32),
            vmem((units, tok, LANES), F32),
            vmem((units, tok, LANES), F32),
            vmem((ranks - 1, tiles, tok, LANES), F32),
            vmem((ranks - 1, tiles, tok, LANES), F32),
            dma((ranks,)), dma((ranks,)),
            pair(), pair(), pair(), pair(), pair(), pair(),
            dma((inner_count - 1,)), dma((inner_count - 1,)),
            dma((inner_count - 1,)), dma((inner_count - 1,)),
            dma((outer_count - 1,)), dma((outer_count - 1,)),
            dma((ranks - 1, tiles)), dma((ranks - 1, tiles)),
        ],
        compiler_params=pltpu.CompilerParams(
            collective_id=0, has_side_effects=True, vmem_limit_bytes=32 * 1024 * 1024),
    )(*(pltpu.with_memory_space_constraint(array, pltpu.HBM) for array in (
        queries, keys, values, pool_fine.T, pool_coarse)))
    return pl.pallas_call(
        norm_kernel,
        out_shape=jax.ShapeDtypeStruct((tok, HQ * HD), BF16),
        in_specs=[pl.BlockSpec(memory_space=pltpu.VMEM)] * 2,
        out_specs=pl.BlockSpec(memory_space=pltpu.VMEM),
        compiler_params=pltpu.CompilerParams(vmem_limit_bytes=8 * 1024 * 1024),
    )(attended, gain.reshape(1, -1))


def solution(mesh):
    rows = P(("outer", "inner"), None)
    return jax.shard_map(
        functools.partial(local, mesh.shape["outer"], mesh.shape["inner"]),
        mesh=mesh, in_specs=(rows, rows, rows, P(), P(), P()),
        out_specs=rows, check_vma=False,
    )
```

```python
import functools
import math

import jax
import jax.numpy as jnp
from jax import lax
from jax.experimental import pallas as pl
from jax.experimental.pallas import tpu as pltpu
from jax.sharding import PartitionSpec as P

HQ = 16
KVH = 4
HD = 64
BLOCK = 512
FINE = 16
RATIO = 8
COARSE = 128

EPSILON = 1e-06
MASKED_SCORE = -1e30
LANES = 128
MESH = pl.DeviceIdType.MESH
BF16 = jnp.bfloat16
F32 = jnp.float32


def kernel(
    outer_count, inner_count,
    q_hbm, k_hbm, v_hbm, pf_hbm, pc_hbm, out_ref,
    q_ref, k_ref, v_ref, pf_ref, pc_ref, in_sems,
    q_all, own_k, own_v, mate_k, mate_v, other_k, other_v,
    ka, va, kb, vb, kc, vc, bias_ref,
    fine_send, fine_all, coarse_send, coarse_pad, coarse_group, coarse_all,
    peaks, sums, att_send, att_recv,
    q_ss, q_rs, own_ss, own_rs, mate_ss, mate_rs, other_ss, other_rs,
    fine_ss, fine_rs, cg_ss, cg_rs, co_ss, co_rs, att_ss, att_rs,
):
    tok = q_ref.shape[0]
    ranks = BLOCK // tok
    kv_width = KVH * HD
    share = kv_width // ranks
    q_share = HQ * HD // ranks
    tiles = q_share // LANES
    kv_local = share // HD
    tiles_per_kv = tiles // kv_local
    rows_kv = tiles_per_kv * tok
    fine_dev = tok // FINE
    coarse_dev = tok // COARSE
    group_tok = tok * inner_count
    fine_amount = group_tok // FINE
    coarse_amount = outer_count * group_tok // COARSE
    blocks = outer_count * inner_count // ranks
    factor = HD ** (-0.5) * math.log2(math.e)

    o_me = lax.axis_index("outer")
    i_me = lax.axis_index("inner")
    linear = o_me * inner_count + i_me
    block = linear // ranks
    rank = lax.rem(linear, ranks)
    odd = lax.rem(block, 2)
    mate = block + 1 - 2 * odd
    relay_from = block - 2 + 4 * odd
    relay_to = block + 2 - 4 * odd
    has_other = (relay_from >= 0) & (relay_from < blocks)
    has_next = (relay_to >= 0) & (relay_to < blocks)

    def at_rank(which_block, rel):
        target_rank = lax.rem(rank + rel, ranks)
        spot = which_block * ranks + target_rank
        return (spot // inner_count, lax.rem(spot, inner_count)), target_rank

    inner_peers = [lax.rem(i_me + rel, inner_count) for rel in range(1, inner_count)]
    outer_peers = [lax.rem(o_me + rel, outer_count) for rel in range(1, outer_count)]

    loads = [
        pltpu.make_async_copy(src, dst, in_sems.at[n])
        for n, (src, dst) in enumerate((
            (k_hbm, k_ref), (q_hbm, q_ref), (v_hbm, v_ref), (pf_hbm, pf_ref), (pc_hbm, pc_ref)))
    ]
    for load in loads:
        load.start()

    barrier = pltpu.get_barrier_semaphore()

    def greet(device):
        pl.semaphore_signal(barrier, inc=1, device_id=device, device_id_type=MESH)

    for peer in inner_peers:
        greet((o_me, peer))
    for peer in outer_peers:
        greet((peer, i_me))
    for rel in range(ranks):
        greet(at_rank(mate, rel)[0])

    for which in (relay_from, relay_to):
        greet(at_rank(lax.rem(which + blocks, blocks), 0)[0])

    for load in loads:
        load.wait()

    def remote(src, dst, send_sem, recv_sem, device):
        return pltpu.make_async_remote_copy(
            src_ref=src, dst_ref=dst, send_sem=send_sem, recv_sem=recv_sem,
            device_id=device, device_id_type=MESH,
        )

    def cols(index, width):
        return pl.ds(pl.multiple_of(index * width, LANES), width)

    own_copies = []
    for rel in range(1, ranks):
        device, target = at_rank(block, rel)
        slot = ranks - rel
        own_copies.append(remote(
            k_ref.at[:, cols(target, share)], own_k.at[slot],
            own_ss.at[0, slot], own_rs.at[0, slot], device))
        own_copies.append(remote(
            q_ref.at[:, cols(target, q_share)], q_all.at[slot],
            q_ss.at[slot], q_rs.at[slot], device))
        own_copies.append(remote(
            v_ref.at[:, cols(target, share)], own_v.at[slot],
            own_ss.at[1, slot], own_rs.at[1, slot], device))

    def mate_copies_of(part, src, dst):
        made = []
        for rel in range(ranks):
            device, target = at_rank(mate, rel)
            slot = (ranks - rel) % ranks
            made.append(remote(
                src.at[:, cols(target, share)], dst.at[slot],
                mate_ss.at[part, slot], mate_rs.at[part, slot], device))
        return made

    def relay_copies(part):
        device = at_rank(relay_to, 0)[0]
        src, dst = ((mate_k, other_k), (mate_v, other_v))[part]
        return [remote(src.at[slot], dst.at[slot], other_ss.at[part, slot],
                       other_rs.at[part, slot], device) for slot in range(ranks)]

    mate_k_copies = mate_copies_of(0, k_ref, mate_k)
    mate_v_copies = mate_copies_of(1, v_ref, mate_v)

    def spread(pool):
        rows = pool.shape[0]
        return jnp.concatenate(
            [jnp.broadcast_to(pool[:, n:n + 1], (rows, HD)) for n in range(2 * KVH)], axis=1)

    pf = spread(pf_ref[...].T)
    pc = spread(pc_ref[...])
    paired = jnp.concatenate([k_ref[...], v_ref[...]], axis=1).astype(F32)
    fine = jnp.sum(paired.reshape(fine_dev, FINE, 2 * kv_width) * pf[None], axis=1).astype(BF16)
    fine_wide = fine.astype(F32)
    coarse = jnp.sum(
        fine_wide.reshape(coarse_dev, RATIO, 2 * kv_width) * pc[None], axis=1).astype(BF16)
    padded = -(-coarse_dev // 8) * 8
    coarse_wide = coarse.astype(F32)
    if padded > coarse_dev:
        coarse_wide = jnp.concatenate(
            [coarse_wide, jnp.zeros((padded - coarse_dev, 2 * kv_width), F32)], axis=0)
    for n in range(ranks):
        k_cols = slice(n * share, (n + 1) * share)
        v_cols = slice(kv_width + n * share, kv_width + (n + 1) * share)
        fine_send[n] = jnp.concatenate([fine[:, k_cols], fine[:, v_cols]], axis=1)
        coarse_send[n] = jnp.concatenate([coarse_wide[:, k_cols], coarse_wide[:, v_cols]], axis=1)
    fine_all[i_me] = fine_send[rank]
    coarse_pad[i_me] = coarse_send[rank]

    group_copies = []
    for n, peer in enumerate(inner_peers):
        peer_rank = lax.rem(peer, ranks)
        group_copies.append(remote(
            coarse_send.at[peer_rank], coarse_pad.at[i_me],
            cg_ss.at[n], cg_rs.at[n], (o_me, peer)))
        group_copies.append(remote(
            fine_send.at[peer_rank], fine_all.at[i_me],
            fine_ss.at[n], fine_rs.at[n], (o_me, peer)))

    low = (lax.broadcasted_iota(jnp.int32, (1, LANES), 1) < HD).astype(F32).astype(BF16)
    high = (lax.broadcasted_iota(jnp.int32, (1, LANES), 1) >= HD).astype(F32).astype(BF16)

    def variants(k_raw, v_raw, k_out, v_out, rows):
        k_swap = pltpu.roll(k_raw.astype(F32), HD, 1).astype(BF16)
        v_swap = pltpu.roll(v_raw.astype(F32), HD, 1).astype(BF16)
        for n in range(kv_local):
            at_low = (k_raw, v_raw) if n == 0 else (k_swap, v_swap)
            at_high = (k_swap, v_swap) if n == 0 else (k_raw, v_raw)
            k_out[n, 0, rows, :] = at_low[0] * low
            k_out[n, 1, rows, :] = at_high[0] * high
            v_out[n, 0, rows, :] = at_low[1] * low + high
            v_out[n, 1, rows, :] = at_high[1] * high + low

    def unit(part, n, half, k_set, v_set, span, bias, first):
        query = jnp.concatenate(
            [q_all[part, :, cols(n * tiles_per_kv + x, LANES)] for x in range(tiles_per_kv)],
            axis=0)
        scores = lax.dot_general(
            query, k_set[n, half, span, :], (((1,), (1,)), ((), ())),
            preferred_element_type=F32)
        if bias is not None:
            scores = scores + bias
        peak = jnp.broadcast_to(jnp.max(scores, axis=1, keepdims=True), (rows_kv, LANES))
        at = (part * kv_local + n) * 2 + half
        if not first:
            before = peaks[at]
            peak = jnp.maximum(peak, before)
        wide = jnp.concatenate([peak] * (scores.shape[1] // LANES), axis=1)
        weights = jnp.exp2((scores - wide) * factor).astype(BF16)
        blended = jnp.dot(weights, v_set[n, half, span, :], preferred_element_type=F32)
        if not first:
            blended = blended + sums[at] * jnp.exp2((before - peak) * factor)
        return at, peak, blended

    def stage(start, stop, k_set, v_set, span, first):
        def body(step, carry):
            part = start + step // kv_local
            n = lax.rem(step, kv_local)
            for at, peak, blended in [
                unit(part, n, half, k_set, v_set, span, None, first) for half in range(2)
            ]:
                peaks[at] = peak
                sums[at] = blended
            return carry
        lax.fori_loop(0, (stop - start) * kv_local, body, 0)

    q_all[0] = q_ref[:, cols(rank, q_share)]
    variants(k_ref[:, cols(rank, share)], v_ref[:, cols(rank, share)], ka, va, slice(0, tok))
    stage(0, 1, ka, va, slice(0, tok), True)

    pl.semaphore_wait(barrier, inner_count - 1 + outer_count - 1 + ranks + 2)
    for copy in own_copies + mate_k_copies + group_copies + mate_v_copies:
        copy.start()

    for copy in own_copies:
        copy.wait_recv()
    for slot in range(1, ranks):
        variants(own_k[slot], own_v[slot], ka, va, slice(slot * tok, (slot + 1) * tok))
        variants(own_k[slot], own_v[slot], kb, vb, slice((slot - 1) * tok, slot * tok))

    stage(1, ranks, ka, va, slice(0, BLOCK), True)

    for copy in group_copies:
        copy.wait_recv()
    for n in range(inner_count):
        coarse_group[n * coarse_dev:(n + 1) * coarse_dev, :] = coarse_pad[n, 0:coarse_dev, :]
    coarse_all[o_me] = coarse_group[...]
    outer_copies = []
    for n, peer in enumerate(outer_peers):
        outer_copies.append(remote(
            coarse_group, coarse_all.at[o_me], co_ss.at[n], co_rs.at[n], (peer, i_me)))
    for copy in outer_copies:
        copy.start()

    for part, copies in enumerate((mate_k_copies, mate_v_copies)):
        for copy in copies:
            copy.wait_recv()

        @pl.when(has_next)
        def _():
            for copy in relay_copies(part):
                copy.start()
    for slot in range(ranks):
        variants(mate_k[slot], mate_v[slot], kb, vb,
                 slice(BLOCK + (slot - 1) * tok, BLOCK + slot * tok))
    stage(0, 1, kb, vb, slice(0, 2 * BLOCK - tok), False)
    stage(1, ranks, kb, vb, slice(BLOCK - tok, 2 * BLOCK - tok), False)

    for copy in outer_copies:
        copy.wait_recv()
    fine_rows = fine_all[...].reshape(fine_amount, 2 * share)
    variants(fine_rows[:, :share], fine_rows[:, share:], kc, vc, slice(BLOCK, BLOCK + fine_amount))
    coarse_rows = coarse_all[...].reshape(coarse_amount, 2 * share).astype(BF16)
    variants(coarse_rows[:, :share], coarse_rows[:, share:], kc, vc,
             slice(BLOCK + fine_amount, BLOCK + fine_amount + coarse_amount))
    far = fine_amount + coarse_amount
    spot = lax.broadcasted_iota(jnp.int32, (1, far), 1)
    fine_pos = o_me * group_tok + spot * FINE
    coarse_pos = (spot - fine_amount) * COARSE
    position = jnp.where(spot < fine_amount, fine_pos, coarse_pos)
    distance = jnp.abs(lax.div(position, BLOCK) - block)
    outside = (spot < fine_amount) | (lax.div(position, group_tok) != o_me)
    bias_ref[:, BLOCK:] = jnp.where((distance > 1) & outside, 0.0, MASKED_SCORE)

    @pl.when(has_other)
    def _():
        for copy in relay_copies(0) + relay_copies(1):
            copy.wait_recv()
        for slot in range(ranks):
            variants(other_k[slot], other_v[slot], kc, vc, slice(slot * tok, (slot + 1) * tok))
        bias_ref[:, :BLOCK] = jnp.zeros((1, BLOCK), F32)

    @pl.when(jnp.logical_not(has_other))
    def _():
        zero = jnp.zeros((BLOCK, LANES), BF16)
        for n in range(kv_local):
            for half in range(2):
                kc[n, half, 0:BLOCK, :] = zero
                vc[n, half, 0:BLOCK, :] = zero
        bias_ref[:, :BLOCK] = jnp.full((1, BLOCK), MASKED_SCORE, F32)

    is_low = lax.broadcasted_iota(jnp.int32, (1, LANES), 1) < HD

    def finish(part, n):
        lower, upper = [
            unit(part, n, half, kc, vc, slice(None), bias_ref[...], False)[2] for half in range(2)]
        totals = pltpu.roll(jnp.where(is_low, upper, lower), HD, 1)
        return jnp.where(is_low, lower, upper) / totals

    def att_copy(part, tile):
        device, _ = at_rank(block, part)
        slot = ranks - part - 1
        return remote(att_send.at[part - 1, tile], att_recv.at[slot, tile],
                      att_ss.at[slot, tile], att_rs.at[slot, tile], device)

    for part in range(1, ranks):
        def give(n, carry):
            attended = finish(part, n)
            for x in range(tiles_per_kv):
                tile = n * tiles_per_kv + x
                att_send[part - 1, tile] = attended[x * tok:(x + 1) * tok]
                att_copy(part, tile).start()
            return carry
        lax.fori_loop(0, kv_local, give, 0)

    def keep(n, carry):
        attended = finish(0, n)
        for x in range(tiles_per_kv):
            tile = n * tiles_per_kv + x
            out_ref[:, cols(rank * tiles + tile, LANES)] = attended[x * tok:(x + 1) * tok]
        return carry

    lax.fori_loop(0, kv_local, keep, 0)
    for part in range(1, ranks):
        slot = ranks - part
        column = lax.rem(rank + slot, ranks) * tiles
        for tile in range(tiles):
            att_copy(part, tile).wait_recv()
            out_ref[:, cols(column + tile, LANES)] = att_recv[slot - 1, tile]

    for copy in own_copies + mate_k_copies + mate_v_copies + group_copies + outer_copies:
        copy.wait_send()

    @pl.when(has_next)
    def _():
        for copy in relay_copies(0) + relay_copies(1):
            copy.wait_send()

    for part in range(1, ranks):
        for tile in range(tiles):
            att_copy(part, tile).wait_send()


def norm_kernel(attended_ref, gain_ref, out_ref):
    attended = attended_ref[...]
    rescale = lax.rsqrt(jnp.mean(attended * attended, axis=1, keepdims=True) + EPSILON)
    out_ref[...] = (attended * rescale * gain_ref[...]).astype(BF16)


def local(outer_count, inner_count, queries, keys, values, pool_fine, pool_coarse, gain):
    tok = queries.shape[0]
    ranks = BLOCK // tok
    share = KVH * HD // ranks
    kv_local = share // HD
    q_share = HQ * HD // ranks
    tiles = q_share // LANES
    group_tok = tok * inner_count
    far = group_tok // FINE + outer_count * group_tok // COARSE
    coarse_dev = tok // COARSE
    padded = -(-coarse_dev // 8) * 8
    assert ranks >= 2 and BLOCK % tok == 0 and kv_local == 2 and share == LANES
    assert inner_count % ranks == 0 and (outer_count * inner_count // ranks) % 2 == 0
    dma = pltpu.SemaphoreType.DMA
    vmem = pltpu.VMEM
    near = lambda: vmem((ranks, tok, share), BF16)
    sets = lambda amount: vmem((kv_local, 2, amount, LANES), BF16)
    units = ranks * kv_local * 2
    rows_kv = tiles // kv_local * tok
    pair = lambda: dma((2, ranks))
    attended = pl.pallas_call(
        functools.partial(kernel, outer_count, inner_count),
        out_shape=jax.ShapeDtypeStruct((tok, HQ * HD), F32),
        in_specs=[pl.BlockSpec(memory_space=pltpu.HBM)] * 5,
        out_specs=pl.BlockSpec(memory_space=pltpu.VMEM),
        scratch_shapes=[
            vmem(queries.shape, BF16), vmem(keys.shape, BF16), vmem(values.shape, BF16),
            vmem(pool_fine.shape[::-1], F32), vmem(pool_coarse.shape, F32), dma((5,)),
            vmem((ranks, tok, q_share), BF16),
            near(), near(), near(), near(), near(), near(),
            sets(BLOCK), sets(BLOCK), sets(2 * BLOCK - tok), sets(2 * BLOCK - tok),
            sets(BLOCK + far), sets(BLOCK + far), vmem((1, BLOCK + far), F32),
            vmem((ranks, tok // FINE, 2 * share), BF16),
            vmem((inner_count, tok // FINE, 2 * share), BF16),
            vmem((ranks, padded, 2 * share), F32),
            vmem((inner_count, padded, 2 * share), F32),
            vmem((inner_count * coarse_dev, 2 * share), F32),
            vmem((outer_count, inner_count * coarse_dev, 2 * share), F32),
            vmem((units, rows_kv, LANES), F32),
            vmem((units, rows_kv, LANES), F32),
            vmem((ranks - 1, tiles, tok, LANES), F32),
            vmem((ranks - 1, tiles, tok, LANES), F32),
            dma((ranks,)), dma((ranks,)),
            pair(), pair(), pair(), pair(), pair(), pair(),
            dma((inner_count - 1,)), dma((inner_count - 1,)),
            dma((inner_count - 1,)), dma((inner_count - 1,)),
            dma((outer_count - 1,)), dma((outer_count - 1,)),
            dma((ranks - 1, tiles)), dma((ranks - 1, tiles)),
        ],
        compiler_params=pltpu.CompilerParams(
            collective_id=0, has_side_effects=True, vmem_limit_bytes=32 * 1024 * 1024),
    )(*(pltpu.with_memory_space_constraint(array, pltpu.HBM) for array in (
        queries, keys, values, pool_fine.T, pool_coarse)))
    return pl.pallas_call(
        norm_kernel,
        out_shape=jax.ShapeDtypeStruct((tok, HQ * HD), BF16),
        in_specs=[pl.BlockSpec(memory_space=pltpu.VMEM)] * 2,
        out_specs=pl.BlockSpec(memory_space=pltpu.VMEM),
        compiler_params=pltpu.CompilerParams(vmem_limit_bytes=8 * 1024 * 1024),
    )(attended, gain.reshape(1, -1))


def solution(mesh):
    rows = P(("outer", "inner"), None)
    return jax.shard_map(
        functools.partial(local, mesh.shape["outer"], mesh.shape["inner"]),
        mesh=mesh, in_specs=(rows, rows, rows, P(), P(), P()),
        out_specs=rows, check_vma=False,
    )
```
